32 devices in a mesh: row: 8 (over z, x), col: 4 (over y, core).
Axes of the slice: x: 2, y: 2, z: 4, core: 2. Of those that a mesh axis runs over, the one named last changes fastest.
Arguments:
- queue: float32 [4096, 256], P(('row', 'col')), may hold values from -12 to 12
Outputs:
- queue_grad: float32 [4096, 256], P(('row', 'col'))
- loss: float32 [], replicated
The draws below stay inside these ranges and needn't reach their ends.
All inputs are finite; a program needn't handle non-finite values.
Results may differ from the reference program's by a relative error of at most 0.0025.
The reference program's roundings to bfloat16 on the way (of `unit_low`) count: a program that leaves them out, or rounds other values in their place, can miss the bound.
Values may be sent and summed in bfloat16 or wider, within the bound.
No kernel may reach another device: no remote copies, remote signals or barrier semaphores. Data moves between devices by JAX's collectives and lax.ppermute only.
A program may use at most 64 MiB of HBM per device.

```python
import math
import jax
import jax.numpy as jnp
from jax import lax

E = 256
QUEUE = 4096


def draw_queue(key, part):
    keys = jax.random.split(jax.random.fold_in(key, 11), 6)
    centres = jax.random.normal(keys[0], (64, E), jnp.float32)
    labels = jax.random.randint(keys[1], (QUEUE,), 0, 64)
    picked = jnp.dot(jax.nn.one_hot(labels, 64, dtype=jnp.float32), centres)
    position = jnp.arange(QUEUE, dtype=jnp.float32)[:, None] / QUEUE
    mixing = 0.4 * jnp.exp(position * jnp.log(8.0)) * jnp.exp(jax.random.uniform(keys[2], (QUEUE, 1), jnp.float32, -0.35, 0.35))
    noise = jax.random.normal(keys[3], (QUEUE, E), jnp.float32)
    scaling = jnp.exp(jax.random.uniform(keys[5], (QUEUE, 1), jnp.float32, -0.7, 0.7))
    return jnp.clip(scaling * (mixing * picked + noise), -12.0, 12.0)


def setup_inputs(seed: int = 0) -> dict:
    streams_of = jax.random.split(jax.random.key(seed), 2)
    return {
        "queue": draw_queue(jax.random.fold_in(streams_of[1], 71), 0),
    }


def reference(queue):
    row_norm = jnp.sqrt(lax.optimization_barrier(jnp.sum(queue * queue, axis=1, keepdims=True)) + 1e-06)
    unit = queue / row_norm
    unit_low = unit.astype(jnp.bfloat16)
    unit_wide = unit_low.astype(jnp.float32)
    squares = lax.optimization_barrier(jnp.sum(unit_wide * unit_wide, axis=1))
    step_rows = math.gcd(QUEUE, 512)
    ident_all = jnp.arange(QUEUE, dtype=jnp.int32)

    def one_block(index):
        start = (index * step_rows).astype(jnp.int32)
        rows_low = lax.dynamic_slice_in_dim(unit_low, start, step_rows, 0)
        rows_sq = lax.dynamic_slice_in_dim(squares, start, step_rows, 0)
        inner = jnp.dot(rows_low, unit_low.T, preferred_element_type=jnp.float32)
        dist = rows_sq[:, None] + squares[None, :] - 2.0 * inner
        ident_rows = start + jnp.arange(step_rows, dtype=jnp.int32)
        weight = jnp.where(ident_rows[:, None] != ident_all[None, :], jnp.exp(-2.0 * dist), jnp.zeros_like(dist))
        pulled = jnp.dot(weight.astype(jnp.bfloat16), unit_low, preferred_element_type=jnp.float32)
        return (jnp.sum(weight), lax.optimization_barrier(jnp.sum(weight, axis=1)), pulled)
    totals, row_sums, pulled = lax.map(one_block, jnp.arange(QUEUE // step_rows, dtype=jnp.int32))
    total = jnp.sum(totals)
    row_sums = row_sums.reshape(QUEUE)
    pulled = pulled.reshape(QUEUE, E)
    grad_unit = -8.0 * QUEUE * (unit_wide * row_sums[:, None] - pulled) / total
    queue_grad = (grad_unit - unit * lax.optimization_barrier(jnp.sum(unit * grad_unit, axis=1, keepdims=True))) / row_norm
    loss = jnp.log(total / (QUEUE * (QUEUE - 1.0)))
    return (queue_grad, loss)
```

```python
import math

import jax
import jax.numpy as jnp
from jax import lax
from jax.experimental import pallas as pl
from jax.experimental.pallas import tpu as pltpu
from jax.sharding import PartitionSpec as P

LOG2E = math.log2(math.e)
AXES = ("row", "col")
TILE = 256
VMEM = pl.BlockSpec(memory_space=pltpu.VMEM)
SMEM = pl.BlockSpec(memory_space=pltpu.SMEM)


def prep_kernel(queue_ref, unit_ref, low_ref, norm_ref):
    queue = queue_ref[...]
    norm = jnp.sqrt(jnp.sum(queue * queue, axis=1, keepdims=True) + 1e-06)
    unit = queue / norm
    unit_ref[...] = unit
    low_ref[...] = unit.astype(jnp.bfloat16)
    norm_ref[...] = jnp.broadcast_to(norm, norm_ref.shape)


def dot_nt(a, b):
    return lax.dot_general(a, b, (((1,), (1,)), ((), ())), preferred_element_type=jnp.float32)


def pairs_kernel(core_ref, mine_ref, other_ref, terms_ref, total_ref, col_ref, row_ref):
    refs = (mine_ref, other_ref)
    rows = mine_ref.shape[0]
    own = terms_ref.shape[0]
    core = core_ref[0]
    for side in range(2):
        for block in range(rows // 128):
            wide = refs[side][pl.ds(block * 128, 128), :].astype(jnp.float32)
            scaled = jnp.sum(wide * wide, axis=1, keepdims=True) * (-2.0 * LOG2E)
            spread = jnp.broadcast_to(scaled, (128, 128))
            col_ref[side, pl.ds(block * 128, 128), :] = spread
            row_ref[side, :, pl.ds(block * 128, 128)] = spread.T[0:8]

    def weights(rows_a, col_a, side, start):
        b = refs[side][pl.ds(start, TILE), :]
        inner = dot_nt(rows_a, b)
        row_b = row_ref[side, 0:1, pl.ds(start, TILE)]
        return jnp.exp2(inner * (4.0 * LOG2E) + (row_b + jnp.concatenate([col_a, col_a], axis=1))), b

    def fold(weight):
        return jnp.sum(weight.reshape(TILE // 8, 8, TILE), axis=0)

    single = jnp.zeros((8, TILE), jnp.float32)
    double = jnp.zeros((8, TILE), jnp.float32)
    tiles = rows // TILE
    per_line = tiles // 4
    for p in range(tiles):
        rows_a = mine_ref[pl.ds(p * TILE, TILE), :]
        col_a = col_ref[0, pl.ds(p * TILE, TILE), :]
        single = single + fold(weights(rows_a, col_a, 0, p * TILE)[0])
        for q in range(p + 1, tiles):
            double = double + fold(weights(rows_a, col_a, 0, q * TILE)[0])
        line, half = divmod(p, per_line)
        near = pl.multiple_of((line * per_line + (half + core) % per_line) * TILE, TILE)
        double = double + fold(weights(rows_a, col_a, 1, near)[0])
        for q in range((line + 1) * per_line, tiles):
            double = double + fold(weights(rows_a, col_a, 1, q * TILE)[0])
    both = single + 2.0 * double
    total_ref[...] = both[:, 0:128] + both[:, 128:256]

    own_rows = mine_ref[0:own, :]
    own_col = col_ref[0, 0:own, :]
    sums = jnp.zeros((own, TILE), jnp.float32)
    pulled = jnp.zeros(terms_ref.shape, jnp.float32)
    for side in range(2):
        for q in range(tiles):
            weight, b = weights(own_rows, own_col, side, q * TILE)
            sums = sums + weight
            pulled = pulled + jnp.dot(weight.astype(jnp.bfloat16), b, preferred_element_type=jnp.float32)
    terms_ref[...] = own_rows.astype(jnp.float32) * jnp.sum(sums, axis=1, keepdims=True) - pulled


def final_kernel(queue_rows, unit_ref, norm_ref, terms_ref, mine_ref, other_ref, grad_ref, loss_ref):
    total = jnp.sum(mine_ref[...] + other_ref[...], keepdims=True) - queue_rows
    unit = unit_ref[...]
    grad_unit = terms_ref[...] * (-8.0 * queue_rows / total)
    radial = jnp.sum(unit * grad_unit, axis=1, keepdims=True)
    grad_ref[...] = (grad_unit - unit * radial) / norm_ref[:, 0:1]
    loss_ref[0] = jnp.log(total / (queue_rows * (queue_rows - 1.0)))[0, 0]


def permute(value, flip):
    count = lax.axis_size("row") * lax.axis_size("col")
    return lax.ppermute(value, AXES, [(i, i ^ flip) for i in range(count)])


def fast_device(queue):
    own, width = queue.shape
    devices = lax.axis_size("row") * lax.axis_size("col")
    queue_rows = float(own * devices)
    f32 = jnp.float32
    unit, low, norm = pl.pallas_call(
        prep_kernel,
        in_specs=[VMEM],
        out_specs=[VMEM] * 3,
        out_shape=[
            jax.ShapeDtypeStruct((own, width), f32),
            jax.ShapeDtypeStruct((own, width), jnp.bfloat16),
            jax.ShapeDtypeStruct((own, 128), f32),
        ],
        name="prep",
    )(queue)
    z_all = [low, permute(low, 8), permute(low, 16), permute(low, 24)]
    line = jnp.concatenate(z_all, axis=0)
    x_line = permute(line, 4)
    y_line = permute(line, 2)
    half = line.shape[0] // 2
    diag = jnp.concatenate([permute(y_line[:half], 4), permute(x_line[half:], 2)], axis=0)
    mine = jnp.concatenate([line, x_line, y_line, diag], axis=0)
    other = permute(mine, 1)
    core = (lax.axis_index("col") % 2).astype(jnp.int32).reshape(1)
    rows = mine.shape[0]
    terms, part = pl.pallas_call(
        pairs_kernel,
        in_specs=[SMEM, VMEM, VMEM],
        out_specs=[VMEM] * 2,
        out_shape=[jax.ShapeDtypeStruct((own, width), f32), jax.ShapeDtypeStruct((8, 128), f32)],
        scratch_shapes=[pltpu.VMEM((2, rows, 128), f32), pltpu.VMEM((2, 8, rows), f32)],
        name="pairs",
    )(core, mine, other)
    part_other = permute(part, 1)

    def final(*refs):
        final_kernel(queue_rows, *refs)

    grad, loss = pl.pallas_call(
        final,
        in_specs=[VMEM] * 5,
        out_specs=[VMEM, SMEM],
        out_shape=[jax.ShapeDtypeStruct((own, width), f32), jax.ShapeDtypeStruct((1,), f32)],
        name="final",
    )(unit, norm, terms, part, part_other)
    return grad, loss.reshape(())


def reduce_total(total):
    return lax.psum(total, ("row", "col"))


def reduce_rows(terms):
    return lax.psum_scatter(terms, "col", scatter_dimension=0, tiled=True)


def per_device(queue):
    own_rows = queue.shape[0]
    count_row = lax.axis_size("row")
    count_col = lax.axis_size("col")
    queue_rows = own_rows * count_row * count_col
    row_norm = jnp.sqrt(jnp.sum(queue * queue, axis=1, keepdims=True) + 1e-06)
    unit = queue / row_norm
    unit_low = unit.astype(jnp.bfloat16)
    block_a = lax.all_gather(unit_low, "col", axis=0, tiled=True)
    block_b = lax.all_gather(unit_low, "row", axis=0, tiled=True)
    wide_a = block_a.astype(jnp.float32)
    wide_b = block_b.astype(jnp.float32)
    sq_a = jnp.sum(wide_a * wide_a, axis=1)
    sq_b = jnp.sum(wide_b * wide_b, axis=1)
    index_row = lax.axis_index("row")
    index_col = lax.axis_index("col")
    rows_a = block_a.shape[0]
    rows_b = block_b.shape[0]
    ident_b = jnp.arange(rows_b, dtype=jnp.int32)
    ident_b = (
        ident_b // own_rows * (count_col * own_rows) + index_col * own_rows + ident_b % own_rows
    )
    base_a = index_row * (count_col * own_rows)
    step_rows = math.gcd(rows_a, 512)

    def one_block(carry, index):
        start = index * step_rows
        rows_low = lax.dynamic_slice_in_dim(block_a, start, step_rows, 0)
        rows_wide = lax.dynamic_slice_in_dim(wide_a, start, step_rows, 0)
        rows_sq = lax.dynamic_slice_in_dim(sq_a, start, step_rows, 0)
        inner = jnp.dot(rows_low, block_b.T, preferred_element_type=jnp.float32)
        dist = rows_sq[:, None] + sq_b[None, :] - 2.0 * inner
        ident_rows = base_a + start + jnp.arange(step_rows, dtype=jnp.int32)
        weight = jnp.where(
            ident_rows[:, None] != ident_b[None, :], jnp.exp(-2.0 * dist), jnp.zeros_like(dist)
        )
        weight_low = weight.astype(jnp.bfloat16)
        pulled = jnp.dot(weight_low, block_b, preferred_element_type=jnp.float32)
        terms = rows_wide * jnp.sum(weight, axis=1)[:, None] - pulled
        total, terms_b = carry
        return ((total + jnp.sum(weight), terms_b), terms)

    start_b = jnp.zeros((), jnp.float32)
    (total, terms_b), terms_a = lax.scan(
        one_block,
        (jnp.zeros((), jnp.float32), start_b),
        jnp.arange(rows_a // step_rows, dtype=jnp.int32),
    )
    terms_a = terms_a.reshape(rows_a, block_a.shape[1])
    factor = -8.0 * queue_rows
    grad_unit = reduce_rows(terms_a)
    total = reduce_total(total)
    grad_unit = grad_unit * (factor / total)
    queue_grad = (grad_unit - unit * jnp.sum(unit * grad_unit, axis=1, keepdims=True)) / row_norm
    loss = jnp.log(total / (queue_rows * (queue_rows - 1.0)))
    return (queue_grad, loss)


def solution(mesh):
    sizes = dict(mesh.shape)
    fast = sizes["row"] == 8 and sizes["col"] == 4

    def per_mesh(queue):
        return fast_device(queue) if fast and queue.shape == (128, 256) else per_device(queue)

    return jax.shard_map(
        per_mesh,
        mesh=mesh,
        in_specs=(P(("row", "col"), None),),
        out_specs=(P(("row", "col"), None), P()),
        check_vma=False,
    )
```
